64 devices in a mesh: rep: 8 (over x, y, core), dp: 8 (over z).
Axes of the slice: x: 2, y: 2, z: 8, core: 2. Of those that a mesh axis runs over, the one named last changes fastest.
The devices are a block of a 4x4x8 slice.
Arguments:
- x: bfloat16 [64, 2048, 640], P(('rep', 'dp')), parts along dimension 0
- dy: bfloat16 [64, 2048, 640], P(('rep', 'dp')), parts along dimension 0
- w_gate: bfloat16 [2, 640, 1792], replicated
- w_up: bfloat16 [2, 640, 1792], replicated
- w_down: bfloat16 [2, 1792, 640], replicated
- m_w_gate: float32 [2, 640, 1792], replicated
- m_w_up: float32 [2, 640, 1792], replicated
- m_w_down: float32 [2, 1792, 640], replicated
- v_w_gate: float32 [2, 640, 1792], replicated
- v_w_up: float32 [2, 640, 1792], replicated
- v_w_down: float32 [2, 1792, 640], replicated
Outputs:
- output 1: bfloat16 [16, 640, 1792], P('rep'), parts along dimension 0
- output 2: bfloat16 [16, 640, 1792], P('rep'), parts along dimension 0
- output 3: bfloat16 [16, 1792, 640], P('rep'), parts along dimension 0
- output 4: float32 [16, 640, 1792], P('rep'), parts along dimension 0
- output 5: float32 [16, 640, 1792], P('rep'), parts along dimension 0
- output 6: float32 [16, 1792, 640], P('rep'), parts along dimension 0
- output 7: float32 [16, 640, 1792], P('rep'), parts along dimension 0
- output 8: float32 [16, 640, 1792], P('rep'), parts along dimension 0
- output 9: float32 [16, 1792, 640], P('rep'), parts along dimension 0
There are 8 independent parts. The reference program is written for one: setup_inputs(seed, part) draws one part's arguments, and reference() takes and returns one part's arrays. A program takes and returns all parts, laid end to end along the dimension named above; an argument that names none is the same for every part.
All inputs are finite; a program needn't handle non-finite values.
Results may differ from the reference program's by a relative error of at most 0.02.
Values are sent between devices in bfloat16 or wider.
A program may use at most 768 MiB of HBM per device.

```python
import jax
import jax.numpy as jnp
from jax import lax

SEQUENCES = 8
TOKENS = 2048
D = 640
FF = 1792
LAYERS = 2
NAMES = ("w_gate", "w_up", "w_down")
SHAPES = {"w_gate": (LAYERS, D, FF), "w_up": (LAYERS, D, FF), "w_down": (LAYERS, FF, D)}


def bump(key, n, height):
    away = (jnp.arange(n, dtype=jnp.int32) - jax.random.randint(key, (), 0, n, jnp.int32)) % n
    return jnp.where(away < n // 8, height, 1.0)


def together(key, own, strength):
    shared = jax.random.normal(key, own.shape[1:], jnp.float32)
    return (own + strength * shared) * lax.rsqrt(1 + strength * strength)


def setup_inputs(seed: int = 0, part: int = 0) -> dict:
    kx, kdy, ka, kb, kz, kf, kh, kl, *keys = jax.random.split(jax.random.key(seed), 8 + 3 * len(NAMES))
    kx, kdy, ka, kb = (jax.random.fold_in(k, part) for k in (kx, kdy, ka, kb))
    kw, km, kv = (keys[i::3] for i in range(3))
    shape = (SEQUENCES, TOKENS, D)
    much_x, much_dy = jax.random.uniform(kz, (2,), jnp.float32, 0.0, 1.0)
    loud = 2.0 ** jax.random.uniform(jax.random.fold_in(kz, 1), (), jnp.float32, -1.0, 2.0)
    layers = 2.0 ** jax.random.uniform(kl, (LAYERS, 1, 1), jnp.float32, -1.0, 1.0)
    x = together(ka, jax.random.normal(kx, shape, jnp.float32), much_x) * bump(kf, D, 4.0)
    dy = together(kb, jax.random.normal(kdy, shape, jnp.float32), much_dy)
    drawn = {"x": x.astype(jnp.bfloat16), "dy": (loud * dy * (SEQUENCES * TOKENS) ** -0.5).astype(jnp.bfloat16)}
    for key, name in zip(kw, NAMES, strict=True):
        w = jax.random.normal(key, SHAPES[name], jnp.float32) * SHAPES[name][1] ** -0.5
        drawn[name] = (w * {"w_gate": 1.0, "w_up": bump(kh, FF, 4.0), "w_down": layers}[name]).astype(jnp.bfloat16)
    for key, name in zip(km, NAMES, strict=True):
        drawn[f"m_{name}"] = 0.1 * jax.random.normal(key, SHAPES[name], jnp.float32)
    for key, name in zip(kv, NAMES, strict=True):
        drawn[f"v_{name}"] = jax.random.uniform(key, SHAPES[name], jnp.float32, 0.005, 0.015)
    return drawn


def matmul(a, w):
    return jnp.dot(a, w, preferred_element_type=jnp.float32).astype(jnp.bfloat16)


def normed(h):
    wide = h.astype(jnp.float32)
    scale = lax.rsqrt(jnp.mean(wide**2, -1, keepdims=True) + 1e-6)
    return (wide * scale).astype(jnp.bfloat16)


def layer(h, w):
    a = normed(h)
    gate = jnp.dot(a, w["w_gate"], preferred_element_type=jnp.float32)
    up = jnp.dot(a, w["w_up"], preferred_element_type=jnp.float32)
    return h + matmul((jax.nn.silu(gate) * up).astype(jnp.bfloat16), w["w_down"])


def adamw(w, m, v, g):
    m = 0.9 * m + 0.1 * g
    v = 0.95 * v + 0.05 * g * g
    step = m * lax.rsqrt(v + 1e-8) + 0.1 * w
    return (w - 0.02 * step).astype(jnp.bfloat16), m, v


def stack(weights, h):
    return lax.scan(lambda h, w: (layer(h, w), None), h, weights)[0]


def reference(x, dy, w_gate, w_up, w_down, m_w_gate, m_w_up, m_w_down, v_w_gate, v_w_up, v_w_down):
    weights = dict(zip(NAMES, (w_gate, w_up, w_down), strict=True))

    def take(so_far, sequence):
        h, by_y = sequence
        _, back = jax.vjp(lambda w: stack(w, h), weights)
        return jax.tree.map(lambda total, term: total + term.astype(jnp.float32), so_far, back(by_y)[0]), None

    none_yet = {name: jnp.zeros(w.shape, jnp.float32) for name, w in weights.items()}
    by_weights, _ = lax.scan(take, none_yet, (x, dy))
    gradients = [by_weights[name].astype(jnp.bfloat16).astype(jnp.float32) for name in NAMES]
    new = [
        adamw(w.astype(jnp.float32), m, v, g)
        for w, m, v, g in zip((w_gate, w_up, w_down), (m_w_gate, m_w_up, m_w_down), (v_w_gate, v_w_up, v_w_down), gradients, strict=True)
    ]
    return tuple(one[which] for which in range(3) for one in new)
```

```python
import functools

import jax
import jax.numpy as jnp
from jax import lax
from jax.experimental import pallas as pl
from jax.experimental.pallas import tpu as pltpu
from jax.sharding import PartitionSpec as P


F32, BF16 = jnp.float32, jnp.bfloat16
COLS = 256
ROWS = 1024
VMEM_LIMIT = 60 * 1024 * 1024


def dot(a, b, contract):
    return lax.dot_general(a, b, ((contract[:1], contract[1:]), ((), ())), preferred_element_type=F32)


def params(*semantics):
    return pltpu.CompilerParams(dimension_semantics=semantics, vmem_limit_bytes=VMEM_LIMIT)


def cost(flops, *arrays):
    return pl.CostEstimate(flops=flops, bytes_accessed=sum(a.size * a.dtype.itemsize for a in arrays), transcendentals=0)


def shaped(shape, dtype=BF16):
    return jax.ShapeDtypeStruct(shape, dtype)


def norm_scale(wide):
    return lax.rsqrt(jnp.mean(wide * wide, -1, keepdims=True) + 1e-6)


def forward_kernel(h_ref, wg_ref, wu_ref, wd_ref, next_ref, a_ref, act_ref, acc_ref):
    j = pl.program_id(1)

    @pl.when(j == 0)
    def _():
        wide = h_ref[...].astype(F32)
        a_ref[...] = (wide * norm_scale(wide)).astype(BF16)
        acc_ref[...] = jnp.zeros_like(acc_ref)

    a = a_ref[...]
    gate = dot(a, wg_ref[...], (1, 0))
    up = dot(a, wu_ref[...], (1, 0))
    act = (gate * jax.nn.sigmoid(gate) * up).astype(BF16)
    act_ref[...] = act
    acc_ref[...] += dot(act, wd_ref[...], (1, 0))

    @pl.when(j == pl.num_programs(1) - 1)
    def _():
        down = acc_ref[...].astype(BF16).astype(F32)
        next_ref[...] = (h_ref[...].astype(F32) + down).astype(BF16)


def forward(h, wg, wu, wd, number):
    tokens, d = h.shape
    ff = wg.shape[2]
    rows = min(tokens, ROWS)
    by_rows = pl.BlockSpec((rows, d), lambda i, j: (i, 0))
    into = pl.BlockSpec((None, d, COLS), lambda i, j: (number, 0, j))
    out_of = pl.BlockSpec((None, COLS, d), lambda i, j: (number, j, 0))
    return pl.pallas_call(
        forward_kernel,
        grid=(tokens // rows, ff // COLS),
        in_specs=[by_rows, into, into, out_of],
        out_specs=[by_rows, by_rows, pl.BlockSpec((rows, COLS), lambda i, j: (i, j))],
        out_shape=[shaped((tokens, d)), shaped((tokens, d)), shaped((tokens, ff))],
        scratch_shapes=[pltpu.VMEM((rows, d), F32)],
        compiler_params=params("parallel", "arbitrary"),
        cost_estimate=cost(6 * tokens * d * ff, h, h, h),
    )(h, wg, wu, wd)


def gate_kernel(n_outs, h_ref, dy_ref, wg_ref, wu_ref, wd_ref, *refs):
    dg_ref, du_ref, a_ref, *act_ref = refs[-n_outs:]
    j = pl.program_id(1)

    @pl.when(j == 0)
    def _():
        wide = h_ref[...].astype(F32)
        a_ref[...] = (wide * norm_scale(wide)).astype(BF16)

    a = a_ref[...]
    gate = dot(a, wg_ref[...], (1, 0))
    up = dot(a, wu_ref[...], (1, 0))
    by_act = dot(dy_ref[...], wd_ref[...], (1, 1)).astype(BF16).astype(F32)
    s = jax.nn.sigmoid(gate)
    silu = gate * s
    if act_ref:
        act_ref[0][...] = (silu * up).astype(BF16)
    du_ref[...] = (by_act * silu).astype(BF16)
    dg_ref[...] = (by_act * up * (s + silu * (1.0 - s))).astype(BF16)


def gate_backward(h, dy, wg, wu, wd, number, with_act, part=0, parts=1, so_far=None):
    tokens, d = h.shape
    ff = wg.shape[2]
    rows = min(tokens // parts, ROWS)
    tiles = tokens // rows // parts
    first = part * tiles
    by_rows = pl.BlockSpec((rows, d), lambda i, j: (i + first, 0))
    into = pl.BlockSpec((None, d, COLS), lambda i, j: (number, 0, j))
    out_of = pl.BlockSpec((None, COLS, d), lambda i, j: (number, j, 0))
    hidden = pl.BlockSpec((rows, COLS), lambda i, j: (i + first, j))
    extra = 1 if with_act else 0
    operands, specs, aliases = [h, dy, wg, wu, wd], [by_rows, by_rows, into, into, out_of], {}
    if so_far is not None:
        aliases = {len(operands) + i: i for i in range(len(so_far))}
        operands, specs = operands + so_far, specs + [pl.BlockSpec(memory_space=pl.ANY)] * len(so_far)
    return pl.pallas_call(
        functools.partial(gate_kernel, 3 + extra),
        grid=(tiles, ff // COLS),
        in_specs=specs,
        out_specs=[hidden, hidden, by_rows] + [hidden] * extra,
        out_shape=[shaped((tokens, ff)), shaped((tokens, ff)), shaped((tokens, d))] + [shaped((tokens, ff))] * extra,
        input_output_aliases=aliases,
        compiler_params=params("parallel", "arbitrary"),
        cost_estimate=cost(6 * tokens * d * ff // parts, h, h, h),
    )(*operands)


def states_kernel(h_ref, dy_ref, dg_ref, du_ref, wg_ref, wu_ref, *refs):
    out_ref = refs[-1]
    by_a = dot(dg_ref[...], wg_ref[...], (1, 1)) + dot(du_ref[...], wu_ref[...], (1, 1))
    by_a = by_a.astype(BF16).astype(F32)
    wide = h_ref[...].astype(F32)
    scale = norm_scale(wide)
    along = jnp.mean(by_a * wide, -1, keepdims=True)
    by_h = (by_a * scale - wide * (scale * scale * scale * along)).astype(BF16)
    out_ref[...] = (dy_ref[...].astype(F32) + by_h.astype(F32)).astype(BF16)


def states_backward(h, dy, dg, du, wg, wu, number, part=0, parts=1, so_far=None):
    tokens, d = h.shape
    ff = wg.shape[2]
    rows = min(tokens // parts, 512)
    tiles = tokens // rows // parts
    first = part * tiles
    by_rows = pl.BlockSpec((rows, d), lambda i: (i + first, 0))
    hidden = pl.BlockSpec((rows, ff), lambda i: (i + first, 0))
    into = pl.BlockSpec((None, d, ff), lambda i: (number, 0, 0))
    operands, specs, aliases = [h, dy, dg, du, wg, wu], [by_rows, by_rows, hidden, hidden, into, into], {}
    if so_far is not None:
        aliases = {len(operands): 0}
        operands, specs = operands + [so_far], specs + [pl.BlockSpec(memory_space=pl.ANY)]
    return pl.pallas_call(
        states_kernel,
        grid=(tiles,),
        in_specs=specs,
        out_specs=by_rows,
        out_shape=shaped((tokens, d)),
        input_output_aliases=aliases,
        compiler_params=params("parallel"),
        cost_estimate=cost(4 * tokens * d * ff // parts, h, h, h),
    )(*operands)


def weight_kernel(a_ref, b_ref, out_ref):
    out_ref[...] = dot(a_ref[...], b_ref[...], (0, 0)).astype(BF16)


def weight_gradient(a, b):
    tokens, m = a.shape
    n = b.shape[1]
    if n > m:
        grid = (n // COLS,)
        specs = [pl.BlockSpec((tokens, m), lambda j: (0, 0)), pl.BlockSpec((tokens, COLS), lambda j: (0, j))]
        out = pl.BlockSpec((m, COLS), lambda j: (0, j))
    else:
        grid = (m // COLS,)
        specs = [pl.BlockSpec((tokens, COLS), lambda j: (0, j)), pl.BlockSpec((tokens, n), lambda j: (0, 0))]
        out = pl.BlockSpec((COLS, n), lambda j: (j, 0))
    return pl.pallas_call(
        weight_kernel,
        grid=grid,
        in_specs=specs,
        out_specs=out,
        out_shape=shaped((m, n)),
        compiler_params=params("parallel"),
        cost_estimate=cost(2 * tokens * m * n, a, b),
    )(a, b)


def adamw(w_ref, m_ref, v_ref, g_ref, w_out, m_out, v_out):
    g = g_ref[...].astype(F32)
    m = 0.9 * m_ref[...] + 0.1 * g
    v = 0.95 * v_ref[...] + 0.05 * g * g
    step = m * lax.rsqrt(v + 1e-8) + 0.1 * w_ref[...].astype(F32)
    w_out[...] = (w_ref[...].astype(F32) - 0.02 * step).astype(BF16)
    m_out[...] = m
    v_out[...] = v


def adamw_kernel(ids_ref, gg, gu, gd0, gd1, *refs):
    ins, outs = refs[:9], refs[-9:]
    way = pl.program_id(0)

    def one(which, g_ref):
        adamw(ins[which], ins[3 + which], ins[6 + which], g_ref, outs[which], outs[3 + which], outs[6 + which])

    @pl.when(way == 0)
    def _():
        one(0, gg)
        one(2, gd0)

    @pl.when(way == 1)
    def _():
        one(1, gu)
        one(2, gd1)


def adamw_step(ids, pieces, arrays, so_far, number):
    gg, gu, gd0, _ = pieces
    whole = lambda g: pl.BlockSpec(g.shape, lambda way, ids: (0, 0))
    gate = pl.BlockSpec((None, *gg.shape), lambda way, ids: (number, ids[0], 0))
    up = pl.BlockSpec((None, *gu.shape), lambda way, ids: (number, ids[1], 0))
    down = pl.BlockSpec((None, *gd0.shape), lambda way, ids: (number, 2 * ids[way] + way, 0))
    nine = [gate, up, down] * 3
    in_specs = [whole(g) for g in pieces] + nine
    aliases = {}
    operands = [*pieces, *arrays]
    if so_far is not None:
        in_specs += [pl.BlockSpec(memory_space=pl.ANY)] * 9
        aliases = {1 + len(operands) + i: i for i in range(9)}
        operands += so_far
    return pl.pallas_call(
        adamw_kernel,
        grid_spec=pltpu.PrefetchScalarGridSpec(num_scalar_prefetch=1, grid=(2,), in_specs=in_specs, out_specs=nine),
        out_shape=[shaped(a.shape, a.dtype) for a in arrays],
        input_output_aliases=aliases,
        compiler_params=params("arbitrary"),
        cost_estimate=pl.CostEstimate(flops=4_000_000_000, bytes_accessed=22 * sum(g.size for g in pieces), transcendentals=0),
    )(ids, *operands)


class Reduce:
    def __init__(self, me, n, ways, local, way, parts, part):
        self.me, self.n, self.way, self.pairs = me, n, way, ways[way]
        self.parts, self.part, self.left = parts, part, n - 1
        self.slabs = local.reshape(n * parts, local.shape[0] // (n * parts), local.shape[1])
        self.value = self.own()

    def own(self):
        at = self.n - self.left
        chunk = lax.rem(self.me + 2 * self.n + (-at if self.way == 0 else at), self.n)
        return lax.dynamic_index_in_dim(self.slabs, chunk * self.parts + self.part, 0, False)

    def send(self):
        self.come = lax.ppermute(self.value, "dp", self.pairs)

    def receive(self):
        self.left -= 1
        self.value = (self.come.astype(F32) + self.own().astype(F32)).astype(BF16)


class Gather:
    def __init__(self, value, pairs):
        self.value, self.pairs = value, pairs

    def send(self):
        self.come = lax.ppermute(self.value, "dp", self.pairs)

    def receive(self):
        self.value = self.come


def solution(mesh):
    n = mesh.shape["dp"]
    ways = ([(i, (i + 1) % n) for i in range(n)], [(i, (i - 1) % n) for i in range(n)])

    def step(x, dy, *arrays):
        wg, wu, wd = arrays[:3]
        me = lax.axis_index("dp")

        def slot(rings, kernel):
            for ring in rings:
                ring.send()
            out = kernel()
            for ring in rings:
                ring.receive()
            return out

        def reduce(local, way, parts=1, part=0):
            return Reduce(me, n, ways, local, way, parts, part)

        def both(down):
            return [reduce(down, way, 2, way) for way in (0, 1)]

        def live(*rings):
            return [r for r in rings if r.left > 0]

        h0, by_y = x[0], dy[0]
        h1, a0, act0 = forward(h0, wg, wu, wd, 0)
        dg1, du1, a1, act1 = gate_backward(h1, by_y, wg, wu, wd, 1, True)
        down1 = weight_gradient(act1, by_y)
        rings = both(down1)
        gate1 = slot(live(*rings), lambda: weight_gradient(a1, dg1))
        rings.append(reduce(gate1, 0))
        up1 = slot(live(*rings), lambda: weight_gradient(a1, du1))
        rings.append(reduce(up1, 1))
        by_h = None
        for part in range(2):
            by_h = slot(live(*rings), lambda: states_backward(h1, by_y, dg1, du1, wg, wu, 1, part, 2, by_h))
        hidden = None
        for part in range(2):
            hidden = slot(live(*rings), lambda: list(gate_backward(h0, by_h, wg, wu, wd, 0, False, part, 2, hidden)))
        dg0, du0, _ = hidden
        down0 = slot(live(*rings), lambda: weight_gradient(act0, by_h))
        rings0 = both(down0)
        gate0 = slot(live(*rings, *rings0), lambda: weight_gradient(a0, dg0))
        rings0.append(reduce(gate0, 0))
        up0 = slot(live(*rings, *rings0), lambda: weight_gradient(a0, du0))
        rings0.append(reduce(up0, 1))

        def order(rings):
            return [rings[i] for i in (2, 3, 0, 1)]

        so_far = None
        for number, mine, others in ((1, rings, rings0), (0, rings0, [])):
            while live(*mine):
                slot(live(*mine), lambda: None)
            gathers = [Gather(r.value, ways[r.way]) for r in order(mine)]
            for s in range(n):
                ids = jnp.stack([lax.rem(me + n - s, n), lax.rem(me + s, n)])
                pieces = [g.value for g in gathers]
                ring_steps = live(*others) + (gathers if s < n - 1 else [])
                so_far = slot(ring_steps, lambda: list(adamw_step(ids, pieces, arrays, so_far, number)))
        return tuple(so_far)

    step = jax.shard_map(
        step,
        mesh=mesh,
        in_specs=(P(("rep", "dp"), None, None),) * 2 + (P(None, None, None),) * 9,
        out_specs=(P("rep", None, None),) * 9,
        check_vma=False,
    )
    return step
```

```python
import jax
import jax.numpy as jnp
from jax import lax
from jax.experimental import pallas as pl
from jax.experimental.pallas import tpu as pltpu
from jax.sharding import PartitionSpec as P


F32, BF16 = jnp.float32, jnp.bfloat16
COLS = 256
ROWS = 256
VMEM_LIMIT = 60 * 1024 * 1024


def dot(a, b, contract):
    return lax.dot_general(a, b, ((contract[:1], contract[1:]), ((), ())), preferred_element_type=F32)


def params(*semantics):
    return pltpu.CompilerParams(dimension_semantics=semantics, vmem_limit_bytes=VMEM_LIMIT)


def cost(flops, *arrays):
    return pl.CostEstimate(flops=flops, bytes_accessed=sum(a.size * a.dtype.itemsize for a in arrays), transcendentals=0)


def shaped(shape, dtype=BF16):
    return jax.ShapeDtypeStruct(shape, dtype)


def norm_scale(wide):
    return lax.rsqrt(jnp.mean(wide * wide, -1, keepdims=True) + 1e-6)


def forward_kernel(h_ref, wg_ref, wu_ref, wd_ref, next_ref, a_ref, act_ref):
    wide = h_ref[...].astype(F32)
    a = (wide * norm_scale(wide)).astype(BF16)
    a_ref[...] = a
    for j in range(act_ref.shape[1] // COLS):
        at = slice(j * COLS, (j + 1) * COLS)
        gate = dot(a, wg_ref[:, at], (1, 0))
        up = dot(a, wu_ref[:, at], (1, 0))
        act_ref[:, at] = (gate * jax.nn.sigmoid(gate) * up).astype(BF16)
    down = dot(act_ref[...], wd_ref[...], (1, 0)).astype(BF16).astype(F32)
    next_ref[...] = (h_ref[...].astype(F32) + down).astype(BF16)


def tiles_of(h, width):
    rows = min(h.shape[0], ROWS)
    return h.shape[0] // rows, pl.BlockSpec((rows, width), lambda i: (i, 0))


def matrix(w, number):
    return pl.BlockSpec((None, *w.shape[1:]), lambda i: (number, 0, 0))


def forward(h, wg, wu, wd, number):
    tokens, d = h.shape
    ff = wg.shape[2]
    grid, by_rows = tiles_of(h, d)
    _, hidden = tiles_of(h, ff)
    return pl.pallas_call(
        forward_kernel,
        grid=(grid,),
        in_specs=[by_rows] + [matrix(w, number) for w in (wg, wu, wd)],
        out_specs=[by_rows, by_rows, hidden],
        out_shape=[shaped((tokens, d)), shaped((tokens, d)), shaped((tokens, ff))],
        compiler_params=params("arbitrary"),
        cost_estimate=cost(6 * tokens * d * ff, h, h, h),
    )(h, wg, wu, wd)


def gate_kernel(h_ref, dy_ref, wg_ref, wu_ref, wd_ref, dg_ref, du_ref, a_ref, *act_ref):
    wide = h_ref[...].astype(F32)
    a = (wide * norm_scale(wide)).astype(BF16)
    a_ref[...] = a
    dy = dy_ref[...]
    for j in range(dg_ref.shape[1] // COLS):
        at = slice(j * COLS, (j + 1) * COLS)
        gate = dot(a, wg_ref[:, at], (1, 0))
        up = dot(a, wu_ref[:, at], (1, 0))
        by_act = dot(dy, wd_ref[at, :], (1, 1)).astype(BF16).astype(F32)
        s = jax.nn.sigmoid(gate)
        silu = gate * s
        if act_ref:
            act_ref[0][:, at] = (silu * up).astype(BF16)
        du_ref[:, at] = (by_act * silu).astype(BF16)
        dg_ref[:, at] = (by_act * up * (s + silu * (1.0 - s))).astype(BF16)


def gate_backward(h, dy, wg, wu, wd, number, with_act):
    tokens, d = h.shape
    ff = wg.shape[2]
    grid, by_rows = tiles_of(h, d)
    _, hidden = tiles_of(h, ff)
    extra = 1 if with_act else 0
    return pl.pallas_call(
        gate_kernel,
        grid=(grid,),
        in_specs=[by_rows, by_rows] + [matrix(w, number) for w in (wg, wu, wd)],
        out_specs=[hidden, hidden, by_rows] + [hidden] * extra,
        out_shape=[shaped((tokens, ff)), shaped((tokens, ff)), shaped((tokens, d))] + [shaped((tokens, ff))] * extra,
        compiler_params=params("arbitrary"),
        cost_estimate=cost(6 * tokens * d * ff, h, h, h),
    )(h, dy, wg, wu, wd)


def states_kernel(h_ref, dy_ref, dg_ref, du_ref, wg_ref, wu_ref, out_ref):
    by_a = dot(dg_ref[...], wg_ref[...], (1, 1)) + dot(du_ref[...], wu_ref[...], (1, 1))
    by_a = by_a.astype(BF16).astype(F32)
    wide = h_ref[...].astype(F32)
    scale = norm_scale(wide)
    along = jnp.mean(by_a * wide, -1, keepdims=True)
    by_h = (by_a * scale - wide * (scale * scale * scale * along)).astype(BF16)
    out_ref[...] = (dy_ref[...].astype(F32) + by_h.astype(F32)).astype(BF16)


def states_backward(h, dy, dg, du, wg, wu, number):
    tokens, d = h.shape
    ff = wg.shape[2]
    grid, by_rows = tiles_of(h, d)
    _, hidden = tiles_of(h, ff)
    return pl.pallas_call(
        states_kernel,
        grid=(grid,),
        in_specs=[by_rows, by_rows, hidden, hidden, matrix(wg, number), matrix(wu, number)],
        out_specs=by_rows,
        out_shape=shaped((tokens, d)),
        compiler_params=params("arbitrary"),
        cost_estimate=cost(4 * tokens * d * ff, h, h, h),
    )(h, dy, dg, du, wg, wu)


def weight_gradient(a, b):
    a, b = lax.optimization_barrier((a, b))
    return lax.optimization_barrier(dot(a, b, (0, 0)).astype(BF16))


def adamw(w_ref, m_ref, v_ref, g_ref, w_out, m_out, v_out):
    g = g_ref[...].astype(F32)
    m = 0.9 * m_ref[...] + 0.1 * g
    v = 0.95 * v_ref[...] + 0.05 * g * g
    step = m * lax.rsqrt(v + 1e-8) + 0.1 * w_ref[...].astype(F32)
    w_out[...] = (w_ref[...].astype(F32) - 0.02 * step).astype(BF16)
    m_out[...] = m
    v_out[...] = v


def adamw_kernel(ids_ref, gg, gu, gd0, gd1, *refs):
    ins, outs = refs[:9], refs[-9:]
    way = pl.program_id(0)

    def one(which, g_ref):
        adamw(ins[which], ins[3 + which], ins[6 + which], g_ref, outs[which], outs[3 + which], outs[6 + which])

    @pl.when(way == 0)
    def _():
        one(0, gg)
        one(2, gd0)

    @pl.when(way == 1)
    def _():
        one(1, gu)
        one(2, gd1)


def adamw_step(ids, pieces, arrays, so_far, number):
    gg, gu, gd0, _ = pieces
    whole = lambda g: pl.BlockSpec(g.shape, lambda way, ids: (0, 0))
    gate = pl.BlockSpec((None, *gg.shape), lambda way, ids: (number, ids[0], 0))
    up = pl.BlockSpec((None, *gu.shape), lambda way, ids: (number, ids[1], 0))
    down = pl.BlockSpec((None, *gd0.shape), lambda way, ids: (number, 2 * ids[way] + way, 0))
    nine = [gate, up, down] * 3
    in_specs = [whole(g) for g in pieces] + nine
    aliases = {}
    operands = [*pieces, *arrays]
    if so_far is not None:
        in_specs += [pl.BlockSpec(memory_space=pl.ANY)] * 9
        aliases = {1 + len(operands) + i: i for i in range(9)}
        operands += so_far
    return pl.pallas_call(
        adamw_kernel,
        grid_spec=pltpu.PrefetchScalarGridSpec(num_scalar_prefetch=1, grid=(2,), in_specs=in_specs, out_specs=nine),
        out_shape=[shaped(a.shape, a.dtype) for a in arrays],
        input_output_aliases=aliases,
        compiler_params=params("arbitrary"),
        cost_estimate=pl.CostEstimate(flops=4_000_000_000, bytes_accessed=22 * sum(g.size for g in pieces), transcendentals=0),
    )(ids, *operands)


class Reduce:
    def __init__(self, me, n, ways, local, way, parts, part):
        self.me, self.n, self.way, self.pairs = me, n, way, ways[way]
        self.parts, self.part, self.left = parts, part, n - 1
        self.slabs = local.reshape(n * parts, local.shape[0] // (n * parts), local.shape[1])
        self.value = self.own()

    def own(self):
        at = self.n - self.left
        chunk = lax.rem(self.me + 2 * self.n + (-at if self.way == 0 else at), self.n)
        return lax.dynamic_index_in_dim(self.slabs, chunk * self.parts + self.part, 0, False)

    def send(self):
        self.come = lax.ppermute(self.value, "dp", self.pairs)

    def receive(self):
        self.left -= 1
        self.value = (self.come.astype(F32) + self.own().astype(F32)).astype(BF16)


class Gather:
    def __init__(self, value, pairs):
        self.value, self.pairs = value, pairs

    def send(self):
        self.come = lax.ppermute(self.value, "dp", self.pairs)

    def receive(self):
        self.value = self.come


def solution(mesh):
    n = mesh.shape["dp"]
    ways = ([(i, (i + 1) % n) for i in range(n)], [(i, (i - 1) % n) for i in range(n)])

    def step(x, dy, *arrays):
        wg, wu, wd = arrays[:3]
        me = lax.axis_index("dp")

        def slot(rings, kernel):
            for ring in rings:
                ring.send()
            out = kernel()
            for ring in rings:
                ring.receive()
            if rings:
                for ring, value in zip(rings, lax.optimization_barrier([ring.value for ring in rings]), strict=True):
                    ring.value = value
            return out

        def reduce(local, way, parts=1, part=0):
            return Reduce(me, n, ways, local, way, parts, part)

        def both(down):
            return [reduce(down, way, 2, way) for way in (0, 1)]

        def layer(gate, up, down):
            return [reduce(gate, 0), reduce(up, 1), *both(down)]

        h0, by_y = x[0], dy[0]
        h1, a0, act0 = forward(h0, wg, wu, wd, 0)
        dg1, du1, a1, act1 = gate_backward(h1, by_y, wg, wu, wd, 1, True)
        rings = {1: layer(weight_gradient(a1, dg1), weight_gradient(a1, du1), weight_gradient(act1, by_y))}
        by_h = slot(rings[1], lambda: states_backward(h1, by_y, dg1, du1, wg, wu, 1))
        dg0, du0, _ = slot(rings[1], lambda: gate_backward(h0, by_h, wg, wu, wd, 0, False))
        rings[0] = layer(weight_gradient(a0, dg0), weight_gradient(a0, du0), weight_gradient(act0, by_h))
        so_far, brought = None, {1: None, 0: None}

        def advance(number):
            nonlocal so_far
            if brought[number] is None:
                slot(rings[number], lambda: None)
                if rings[number][0].left == 0:
                    rings[number] = [Gather(r.value, r.pairs) for r in rings[number]]
                    brought[number] = 0
                return
            s = brought[number]
            brought[number] += 1
            ids = jnp.stack([lax.rem(me + n - s, n), lax.rem(me + s, n)])
            pieces = [ring.value for ring in rings[number]]
            going = rings[number] if s < n - 1 else []
            so_far = slot(going, lambda: list(adamw_step(ids, pieces, arrays, so_far, number)))

        while brought[0] != n:
            for number in (1, 0):
                if brought[number] != n:
                    advance(number)
        return tuple(so_far)

    step = jax.shard_map(
        step,
        mesh=mesh,
        in_specs=(P(("rep", "dp"), None, None),) * 2 + (P(None, None, None),) * 9,
        out_specs=(P("rep", None, None),) * 9,
        check_vma=False,
    )
    return step
```
